256 devices in a mesh: dp: 8 (over z_lo, core), cent: 32 (over y, z_hi, x).
Axes of the slice: x: 4, y: 4, z: 8 (z_hi: 2, z_lo: 4; z = z_hi * 4 + z_lo), core: 2. Of those that a mesh axis runs over, the one named last changes fastest.
Arguments:
- embeddings: bfloat16 [32768, 768], P(('dp', 'cent')), may hold values from -20 to 20
- fine_centroids: float32 [16384, 768], P('cent'), may hold values from -8 to 8
- parents: int32 [16384], P('cent'), may hold values from 0 to 2047
- coarse_centroids: float32 [2048, 768], P('cent'), may hold values from -6 to 6
Outputs:
- new_fine: float32 [16384, 768], P('cent')
- new_coarse: float32 [2048, 768], P('cent')
The draws below stay inside these ranges and needn't reach their ends.
All inputs are finite; a program needn't handle non-finite values.
Results may differ from the reference program's by a relative error of at most 0.004.
Values may be sent and summed in bfloat16 or wider, within the bound.
No kernel may reach another device: no remote copies, remote signals or barrier semaphores. Data moves between devices by JAX's collectives and lax.ppermute only.
A program may use at most 64 MiB of HBM per device.

```python
import math
import jax
import jax.numpy as jnp
from jax import lax

D = 768
KC = 2048
K = 16384
TOTAL = 32768


def centroid_table(key):
    base = jnp.clip(jax.random.normal(jax.random.fold_in(key, 11), (K, D), jnp.float32), -5.0, 5.0)
    return base


def draw_fine_centroids(key, part):
    return centroid_table(key).astype(jnp.float32)


def draw_embeddings(key, part):
    rows = jnp.clip(jax.random.normal(jax.random.fold_in(key, 22), (TOTAL, D), jnp.float32), -6.0, 6.0)
    return rows.astype(jnp.bfloat16)


def plant(array, stream_key, low, top_value):
    place = [jax.random.randint(jax.random.fold_in(stream_key, axis), (), 0, length) for axis, length in enumerate(array.shape)]
    main_axis = array.shape.index(max(array.shape))
    next_to = place[:main_axis] + [(place[main_axis] + 1) % array.shape[main_axis]] + place[main_axis + 1:]
    return array.at[tuple(place)].set(low).at[tuple(next_to)].set(top_value)


def block_levels(key, extent, cuts, smallest, high):
    loudness = 1.0
    for axis_at, shards_of in cuts:
        heights = jax.random.uniform(jax.random.fold_in(jax.random.fold_in(key, 6), axis_at), (shards_of,), jnp.float32, smallest / len(cuts), high / len(cuts))
        loudness = loudness * jnp.repeat(jnp.exp(heights), extent[axis_at] // shards_of).reshape((-1,) + (1,) * (len(extent) - 1 - axis_at))
    return loudness


def normal_values(rng, extent, scale, limit, pieces=(), kind=jnp.bfloat16):
    values = jax.random.normal(rng, extent, jnp.float32) * scale
    if len(pieces) > 0:
        values = block_levels(rng, extent, pieces, -0.22, 0.18) * values
    return jnp.clip(values, min=-limit, max=limit).astype(kind)


def setup_inputs(seed: int = 0) -> dict:
    seeds = jax.random.split(jax.random.key(seed), 5)
    return {
        "embeddings": draw_embeddings(jax.random.fold_in(seeds[4], 71), 0),
        "fine_centroids": draw_fine_centroids(jax.random.fold_in(seeds[4], 71), 0),
        "parents": plant(jax.random.randint(seeds[2], (K,), 0, KC), jax.random.fold_in(seeds[2], 1), 0, KC - 1).astype(jnp.int32),
        "coarse_centroids": normal_values(seeds[3], (KC, D), 1.0, 6.0, ((0, 32),), jnp.float32),
    }


sharpness = 0.1
coarse_prior = 16.0


def reference(embeddings, fine_centroids, parents, coarse_centroids):
    narrow = fine_centroids.astype(jnp.bfloat16)
    half_norm = 0.5 * jnp.sum(fine_centroids * fine_centroids, axis=1)
    row_count = embeddings.shape[0]
    block_rows = math.gcd(row_count, 512)
    row_blocks = embeddings.reshape(row_count // block_rows, block_rows, embeddings.shape[1])

    def sum_step(carried, one_block):
        scores = jnp.dot(one_block, narrow.T, preferred_element_type=jnp.float32)
        logits = sharpness * (scores - half_norm[None, :])
        row_peak = jnp.max(logits, axis=1)
        weights = jnp.exp(logits - row_peak[:, None])
        row_mass = jnp.sum(weights, axis=1)
        soft = weights / row_mass[:, None]
        wide_block = one_block.astype(jnp.float32)
        summed = carried[0] + jnp.dot(soft.T, wide_block, precision=lax.Precision.HIGHEST, preferred_element_type=jnp.float32)
        counted = carried[1] + jnp.sum(soft, axis=0)
        return (summed, counted), None

    start_state = (jnp.zeros(fine_centroids.shape, jnp.float32), jnp.zeros((fine_centroids.shape[0],), jnp.float32))
    (fine_sums, fine_counts), _ = lax.scan(sum_step, start_state, row_blocks)
    pooled = fine_centroids + fine_sums
    mass = 1.0 + fine_counts
    new_fine = pooled / mass[:, None]
    coarse_sum = jax.ops.segment_sum(pooled, parents, num_segments=KC)
    coarse_mass = jax.ops.segment_sum(mass, parents, num_segments=KC)
    new_coarse = (coarse_prior * coarse_centroids + coarse_sum) / (coarse_prior + coarse_mass)[:, None]
    return (new_fine, new_coarse)
```

```python
import jax
import jax.numpy as jnp
from jax import lax
from jax.experimental import pallas as pl
from jax.experimental.pallas import tpu as pltpu
from jax.sharding import PartitionSpec as P

KC = 2048
D = 768
PRIOR = 16.0
LOG2E = 1.4426950408889634
SCALE = 0.1 * LOG2E
COARSE_SCALE = 1.0 / 16.0
bf16, f16, f32 = jnp.bfloat16, jnp.float16, jnp.float32


SIZES = {"y": 4, "zh": 2, "x": 4, "zl": 4, "core": 2}
PLACE = {"y": ("cent", 8), "zh": ("cent", 4), "x": ("cent", 1), "zl": ("dp", 2), "core": ("dp", 1)}
EXTENT = {"cent": 32, "dp": 8}


def from_ahead(array, axis, step):
    name, stride = PLACE[axis]
    size = SIZES[axis]
    pairs = []
    for me in range(EXTENT[name]):
        at = me // stride % size
        pairs.append((me + ((at + step) % size - at) * stride, me))
    return lax.ppermute(array, name, pairs)


def place_on(axis):
    name, stride = PLACE[axis]
    return lax.axis_index(name) // stride % SIZES[axis]


def ring_of_four(array, axis):
    return [array] + [from_ahead(array, axis, s) for s in (1, 2, 3)]


def weigh_kernel(n, *refs):
    x_refs, narrow_ref, norm_ref, p_ref, stat_ref = refs[:n], *refs[n:]
    norm = norm_ref[...]
    norm = jnp.concatenate([norm, norm], axis=1)
    for i in range(n):
        cols = slice(256 * i, 256 * i + 256)
        t = lax.dot_general(
            narrow_ref[...], x_refs[i][...], (((1,), (1,)), ((), ())), preferred_element_type=f32
        )
        t = (t - norm) * SCALE
        top = jnp.max(t, axis=0, keepdims=True)
        p = jnp.exp2(t - top)
        p_ref[:, cols] = p
        stat_ref[0:1, cols] = top
        stat_ref[1:2, cols] = jnp.sum(p, axis=0, keepdims=True)


def weigh(xs, narrow, norm):
    n, cents = len(xs), narrow.shape[0]
    rows = 256 * n
    return pl.pallas_call(
        lambda *refs: weigh_kernel(n, *refs),
        out_shape=(
            jax.ShapeDtypeStruct((cents, rows), f32),
            jax.ShapeDtypeStruct((2, rows), f32),
        ),
        cost_estimate=pl.CostEstimate(
            flops=2 * rows * cents * D,
            transcendentals=rows * cents,
            bytes_accessed=2 * rows * D + 2 * cents * D + 4 * rows * cents,
        ),
        compiler_params=pltpu.CompilerParams(vmem_limit_bytes=48 * 1024 * 1024),
    )(*xs, narrow, norm)


def sums_kernel(widths, n, *refs):
    k = len(widths)
    p_refs, w_refs, x_refs = refs[:k], refs[k : 2 * k], refs[2 * k : 2 * k + n]
    out_ref, x_all = refs[2 * k + n :]

    @pl.when(pl.program_id(0) == 0)
    def _():
        for i in range(n):
            x_all[256 * i : 256 * i + 256, :] = x_refs[i][...]

    acc = jnp.zeros((256, D), f32)
    count = jnp.zeros((256, 128), f32)
    at = 0
    for p_ref, w_ref, width in zip(p_refs, w_refs, widths):
        soft = p_ref[...] * w_ref[...]
        high = soft.astype(bf16)
        low = (soft - high.astype(f32)).astype(bf16)
        rows = x_all[at : at + width, :]
        acc = acc + jnp.dot(high, rows, preferred_element_type=f32)
        acc = acc + jnp.dot(low, rows, preferred_element_type=f32)
        for c in range(0, width, 128):
            count = count + soft[:, c : c + 128]
        at += width
    turned = acc.T
    counted = jnp.sum(count.T, axis=0, keepdims=True)
    for half in (0, 1):
        out_ref[half, 0:384, :] = turned[384 * half : 384 * half + 384]
        out_ref[half, 384:400, :] = jnp.broadcast_to(counted, (16, 256))


def weighted_sums(block, ps, ws, xs):
    widths = [p.shape[1] for p in ps]
    rows = sum(widths)
    whole = lambda a: pl.BlockSpec(a.shape, lambda i: (0, 0))
    return pl.pallas_call(
        lambda *refs: sums_kernel(widths, len(xs), *refs),
        grid=(2,),
        in_specs=[pl.BlockSpec((256, w), lambda i: (2 * block + i, 0)) for w in widths]
        + [whole(w) for w in ws]
        + [whole(x) for x in xs],
        out_specs=pl.BlockSpec((2, 400, 256), lambda i: (0, 0, i)),
        out_shape=jax.ShapeDtypeStruct((2, 400, 512), f32),
        scratch_shapes=[pltpu.VMEM((rows, D), bf16)],
        cost_estimate=pl.CostEstimate(
            flops=4 * rows * 512 * D,
            transcendentals=0,
            bytes_accessed=2 * rows * D + 4 * rows * 512 + 4 * 800 * 512,
        ),
        compiler_params=pltpu.CompilerParams(vmem_limit_bytes=48 * 1024 * 1024),
    )(*ps, *ws, *xs)


def merge(a, b):
    top = jnp.maximum(a[0], b[0])
    return top, a[1] * jnp.exp2(a[0] - top) + b[1] * jnp.exp2(b[0] - top)


def merged_over(stat, axis, dim):
    got = [from_ahead(stat, axis, s) for s in (1, 2, 3)]
    parts = [stat] + [jnp.roll(g, s, axis=dim) for s, g in zip((1, 2, 3), got)]
    return jnp.stack(merge(merge(parts[0], parts[1]), merge(parts[2], parts[3])))


def core_sum(sums, core):
    mine = lax.dynamic_index_in_dim(sums, core, 0, keepdims=False)
    other = lax.dynamic_index_in_dim(sums, 1 - core, 0, keepdims=False)
    return mine + from_ahead(other, "core", 1)


def coarse_kernel(pooled_ref, parents_ref, out_ref):
    ids = lax.broadcasted_iota(jnp.int32, (KC, 512), 0)
    hot = (ids == parents_ref[...]).astype(f32).astype(bf16)
    rest = pooled_ref[...]
    total = jnp.zeros((KC, 128), f32)
    for _ in range(3):
        part = rest.astype(bf16)
        rest = rest - part.astype(f32)
        total = total + lax.dot_general(
            hot, part, (((1,), (1,)), ((), ())), preferred_element_type=f32
        )
    out_ref[...] = total


def summed_over(tiles, axis):
    size = SIZES[axis]
    me = place_on(axis)
    narrow = tiles.astype(f16)
    total = lax.dynamic_index_in_dim(tiles, me, 0, keepdims=False)
    for s in range(1, size):
        sent = lax.dynamic_index_in_dim(narrow, (me - s) % size, 0, keepdims=False)
        total = total + from_ahead(sent, axis, s).astype(f32)
    return total


def gathered_over(tile, axis):
    size = SIZES[axis]
    me = place_on(axis)
    parts = [tile] + [from_ahead(tile, axis, s) for s in range(1, size)]
    stacked = jnp.stack(parts + parts)
    return lax.dynamic_slice_in_dim(stacked, (size - me) % size, size, 0)


def local(embeddings, fine, parents, coarse):
    core, zl = place_on("core"), place_on("zl")

    own_narrow = fine.astype(bf16)
    own_norm = 0.5 * jnp.sum(fine * fine, axis=1)
    share = lax.dynamic_slice_in_dim(own_narrow, 256 * core, 256, 0)
    direct = from_ahead(share, "zh", 1)
    relayed = from_ahead(direct, "core", 1)
    first = core == 0
    narrow = jnp.concatenate(
        [jnp.where(first, direct, relayed), jnp.where(first, relayed, direct), own_narrow]
    )
    norm = jnp.concatenate([from_ahead(own_norm, "zh", 1), own_norm])
    norm = jnp.broadcast_to(norm[:, None], (1024, 128))

    halves = (embeddings[:64], embeddings[64:])
    near = [jnp.concatenate(ring_of_four(h, axis)) for h, axis in zip(halves, ("x", "y"))]
    ahead = [from_ahead(b, axis, 1) for b, axis in zip(near, ("y", "x"))]
    behind = [from_ahead(b, axis, 3) for b, axis in zip(near, ("y", "x"))]
    far = [
        jnp.concatenate([from_ahead(a[:128], axis, 1), from_ahead(b[128:], axis, 3)])
        for a, b, axis in zip(ahead, behind, ("y", "x"))
    ]
    groups = [near, [ahead[0], behind[0], ahead[1], behind[1]], far]
    weighed = [weigh(xs, narrow, norm) for xs in groups]

    near_s, mid_s, far_s = (s.reshape(2, -1, 4, 64) for _, s in weighed)
    zero = jnp.stack([near_s[:, 0], mid_s[:, 0], far_s[:, 0], mid_s[:, 1]], axis=1)
    one = jnp.stack([near_s[:, 1], mid_s[:, 2], far_s[:, 1], mid_s[:, 3]], axis=1)
    stat = jnp.stack([zero, one.swapaxes(1, 2)], axis=1)
    total = merged_over(merged_over(stat, "x", 3), "y", 2)
    weight = jnp.exp2(stat[0] - total[0]) / total[1]
    zero, one = weight[0].reshape(4, 256), weight[1].swapaxes(0, 1).reshape(4, 256)
    ws = [
        jnp.concatenate([zero[0], one[0]])[None],
        jnp.concatenate([zero[1], zero[3], one[1], one[3]])[None],
        jnp.concatenate([zero[2], one[2]])[None],
    ]
    ps = [p for p, _ in weighed]
    xs = groups[0] + groups[1] + groups[2]

    away = core_sum(weighted_sums(0, ps, ws, xs), core)
    crossed = from_ahead(away.astype(f16), "zh", 1)
    home = core_sum(weighted_sums(1, ps, ws, xs), core) + crossed.astype(f32)

    tiles = jnp.concatenate(
        [home[:384].reshape(4, 96, 512), jnp.broadcast_to(home[384:][None], (4, 16, 512))], axis=1
    )
    owned = summed_over(tiles * COARSE_SCALE, "zl") / COARSE_SCALE
    mass = 1.0 + owned[96:97]
    first_row = core * 384 + zl * 96
    pooled = lax.dynamic_slice_in_dim(fine, first_row, 96, 1).T + owned[:96]

    new_part = (pooled / mass).astype(f16)
    new_half = gathered_over(new_part, "zl").reshape(384, 512)
    new_fine = gathered_over(new_half, "core").reshape(768, 512).astype(f32).T

    with_mass = jnp.concatenate([pooled, jnp.broadcast_to(mass, (32, 512))]) * COARSE_SCALE
    part = pl.pallas_call(
        coarse_kernel, out_shape=jax.ShapeDtypeStruct((KC, 128), f32)
    )(with_mass, parents[None])
    part = part.reshape(4, 2, 4, 64, 128)
    part = summed_over(part.transpose(2, 0, 1, 3, 4), "x")
    part = summed_over(part, "y")
    part = summed_over(part, "zh") / COARSE_SCALE
    old = lax.dynamic_slice_in_dim(coarse, first_row, 96, 1)
    new_cols = (PRIOR * old + part[:, :96]) / (PRIOR + part[:, 96:97])
    new_half = gathered_over(new_cols, "zl").transpose(1, 0, 2).reshape(64, 384)
    new_coarse = gathered_over(new_half, "core").transpose(1, 0, 2).reshape(64, 768)
    return new_fine, new_coarse


def solution(mesh):
    in_specs = (P(("dp", "cent"), None), P("cent", None), P("cent"), P("cent", None))
    out_specs = (P("cent", None), P("cent", None))
    return jax.shard_map(local, mesh=mesh, in_specs=in_specs, out_specs=out_specs, check_vma=False)
```

```python
import jax
import jax.numpy as jnp
from jax import lax
from jax.experimental import pallas as pl
from jax.experimental.pallas import tpu as pltpu
from jax.sharding import Mesh
from jax.sharding import PartitionSpec as P


KC = 2048
D = 768
PRIOR = 16.0
LOG2E = 1.4426950408889634
SCALE = 0.1 * LOG2E
SENT_SCALE = 1.0 / 16.0
WEIGH_MB = 24
SUMS_MB = 28
bf16, f16, f32 = jnp.bfloat16, jnp.float16, jnp.float32


AXES = {"zl": 4, "core": 2, "y": 4, "zh": 2, "x": 4}


def from_ahead(array, axis, step):
    size = AXES[axis]
    if axis not in ("x", "y"):
        return lax.ppermute(array, axis, [((me + step) % size, me) for me in range(size)])
    pairs = []
    for core in (0, 1):
        for me in range(size):
            source = (me + (step if core == 0 else -step)) % size
            pairs.append((core * size + source, core * size + me))
    return lax.ppermute(array, ("core", axis), pairs)


def ring_of_four(array, axis):
    return [array] + [from_ahead(array, axis, s) for s in (1, 2, 3)]


VMEM = pl.BlockSpec(memory_space=pltpu.VMEM)


def weigh_kernel(first, n, *refs):
    skip = 2 if first else 1
    x_refs, c_refs, norm_ref = refs[skip : skip + n], refs[skip + n : skip + n + 3], refs[skip + n + 3]
    p_ref, stat_ref, x_all, norms = refs[skip + n + 4 :]
    if first:
        stat_ref[...] = refs[1][...]
    norms[512:1024, :] = jnp.broadcast_to(norm_ref[...], (128, 512)).T
    for at, c_ref in ((0, c_refs[0]), (256, c_refs[1])):
        row = c_ref[256:264, :].astype(f32)[0:1]
        row = row[:, 0:256] + row[:, 256:512] + row[:, 512:768]
        norms[at : at + 256, :] = jnp.broadcast_to(row, (128, 256)).T

    spans = ((0, 256), (256, 256), (512, 512))
    for i in range(n):
        x = x_refs[i][...]
        x_all[256 * i : 256 * i + 256, :] = x
        tops = []
        for (at, size), c_ref in zip(spans, c_refs):
            t = lax.dot_general(
                c_ref[0:size, :], x, (((1,), (1,)), ((), ())), preferred_element_type=f32
            )
            norm = norms[at : at + size, :]
            t = (t - jnp.concatenate([norm, norm], axis=1)) * SCALE
            p_ref[i, at : at + size, :] = t
            tops.append(jnp.max(t, axis=0, keepdims=True))
        top = jnp.maximum(jnp.maximum(tops[0], tops[1]), tops[2])
        mass = jnp.zeros((1, 256), f32)
        for at, size in spans:
            p = jnp.exp2(p_ref[i, at : at + size, :] - top)
            p_ref[i, at : at + size, :] = p
            mass = mass + jnp.sum(p, axis=0, keepdims=True)
        stat_ref[0, first + i : first + i + 1, :] = top
        stat_ref[1, first + i : first + i + 1, :] = mass


def weigh(place, first, stats, xs, cs, norm):
    n = len(xs)
    rows = 256 * n
    return pl.pallas_call(
        lambda *refs: weigh_kernel(first, n, *refs),
        in_specs=[pl.BlockSpec(memory_space=pltpu.SMEM)] + [VMEM] * (len(stats) + n + 4),
        out_specs=(VMEM,) * 3,
        out_shape=(
            jax.ShapeDtypeStruct((n, 1024, 256), f32),
            jax.ShapeDtypeStruct((2, 8, 256), f32),
            jax.ShapeDtypeStruct((rows, D), bf16),
        ),
        scratch_shapes=[pltpu.VMEM((1024, 128), f32)],
        cost_estimate=pl.CostEstimate(
            flops=2 * rows * 1024 * D,
            transcendentals=rows * 1024,
            bytes_accessed=2 * rows * D + 2 * 1024 * D + 4 * rows * 1024,
        ),
        compiler_params=pltpu.CompilerParams(vmem_limit_bytes=WEIGH_MB * 1024 * 1024),
    )(place, *stats, *xs, *cs, norm)


PIECES = ((0, 1, 6, 2), (3, 4, 7, 5))


def merge_kernel(rolled, last, *refs):
    parts, out_ref = refs[:4], refs[4]
    for half, pieces in enumerate(PIECES):
        for at, piece in enumerate(pieces):
            tops, masses = [], []
            for s, part in enumerate(parts):
                row = piece if half == rolled else pieces[(at - s) % 4]
                top, mass = part[0, row : row + 1, :], part[1, row : row + 1, :]
                if half == rolled and s:
                    cut = 256 - 64 * s
                    top = jnp.concatenate([top[:, cut:], top[:, :cut]], axis=1)
                    mass = jnp.concatenate([mass[:, cut:], mass[:, :cut]], axis=1)
                tops.append(top)
                masses.append(mass)
            high = jnp.maximum(jnp.maximum(tops[0], tops[1]), jnp.maximum(tops[2], tops[3]))
            total = sum(m * jnp.exp2(t - high) for m, t in zip(masses, tops))
            if last:
                own = refs[5][0, piece : piece + 1, :]
                out_ref[piece : piece + 1, :] = jnp.exp2(own - high) / total
            else:
                out_ref[0, piece : piece + 1, :] = high
                out_ref[1, piece : piece + 1, :] = total


def merge_last_kernel(rolled, *refs):
    merge_kernel(rolled, True, *refs[:4], refs[5], refs[4])


def merged_over(stat, axis, rolled, own=None):
    parts = [stat] + [from_ahead(stat, axis, s) for s in (1, 2, 3)]
    if own is None:
        kernel, shape = (lambda *refs: merge_kernel(rolled, False, *refs)), (2, 8, 256)
    else:
        kernel, shape = (lambda *refs: merge_last_kernel(rolled, *refs)), (8, 256)
        parts.append(own)
    return pl.pallas_call(
        kernel,
        in_specs=[VMEM] * len(parts),
        out_specs=VMEM,
        out_shape=jax.ShapeDtypeStruct(shape, f32),
        compiler_params=pltpu.CompilerParams(vmem_limit_bytes=4 * 1024 * 1024),
    )(*parts)


def sums_kernel(place_ref, p0_ref, p1_ref, w_ref, x0_ref, x1_ref, keep_ref, send_ref, parts, turned):
    core, zh = place_ref[0], place_ref[1]
    first = p0_ref.shape[0]
    for tile in range(4):
        span = slice(256 * tile, 256 * tile + 256)
        count = jnp.zeros((256, 128), f32)
        for i in range(8):
            p = p0_ref[i, span, :] if i < first else p1_ref[i - first, span, :]
            soft = p * w_ref[i : i + 1, :]
            high = soft.astype(bf16)
            parts[0:256, 256 * i : 256 * i + 256] = high
            parts[256:512, 256 * i : 256 * i + 256] = (soft - high.astype(f32)).astype(bf16)
            count = count + (soft[:, :128] + soft[:, 128:])
        both = jnp.dot(parts[:, : 256 * first], x0_ref[...], preferred_element_type=f32)
        both = both + jnp.dot(parts[:, 256 * first :], x1_ref[...], preferred_element_type=f32)
        turned[...] = (both[:256] + both[256:]).T
        counted = jnp.broadcast_to(jnp.sum(count.T, axis=0, keepdims=True), (8, 256))
        if tile < 2:
            block, col = 1 - zh, jnp.bitwise_xor(core, tile)
        else:
            block, col = zh, tile - 2
        lanes = pl.ds(pl.multiple_of(col * 256, 256), 256)
        for ref, half in ((keep_ref, core), (send_ref, 1 - core)):
            for q in range(4):
                part = turned[pl.ds(pl.multiple_of(384 * half + 96 * q, 32), 96), :]
                ref[block, q, 0:96, lanes] = part
                ref[block, q, 96:104, lanes] = counted


def weighted_sums(place, ps, w, xs):
    rows = 2048
    shape = jax.ShapeDtypeStruct((2, 4, 104, 512), f32)
    return pl.pallas_call(
        sums_kernel,
        in_specs=[pl.BlockSpec(memory_space=pltpu.SMEM)] + [VMEM] * 5,
        out_specs=(VMEM, VMEM),
        out_shape=(shape, shape),
        scratch_shapes=[pltpu.VMEM((512, rows), bf16), pltpu.VMEM((D, 256), f32)],
        cost_estimate=pl.CostEstimate(
            flops=8 * rows * 512 * D,
            transcendentals=0,
            bytes_accessed=2 * rows * D + 8 * rows * 512 + 8 * 832 * 512,
        ),
        compiler_params=pltpu.CompilerParams(vmem_limit_bytes=SUMS_MB * 1024 * 1024),
    )(place, *ps, w, *xs)


def coarse_kernel(pooled_ref, parents_ref, out_ref):
    ids = lax.broadcasted_iota(jnp.int32, (KC, 512), 0)
    hot = (ids == parents_ref[...]).astype(f32).astype(bf16)
    pooled = pooled_ref[...]
    high = pooled.astype(bf16)
    low = (pooled - high.astype(f32)).astype(bf16)
    both = lax.dot_general(
        hot,
        jnp.concatenate([high, low]),
        (((1,), (1,)), ((), ())),
        preferred_element_type=f32,
    )
    out_ref[...] = both[:, :128] + both[:, 128:]


def gathered_over(tile, axis):
    size = AXES[axis]
    me = lax.axis_index(axis)
    parts = [tile] + [from_ahead(tile, axis, s) for s in range(1, size)]
    stacked = jnp.stack(parts + parts)
    return lax.dynamic_slice_in_dim(stacked, (size - me) % size, size, 0)


def joined_kernel(place_ref, *refs):
    parts, out_ref, rows = refs[:4], refs[4], refs[5]
    core, zl = place_ref[0], place_ref[2]
    for s in range(4):
        for c in (0, 1):
            piece = parts[s][c]
            at = jnp.bitwise_xor(core, c) * 4 + jnp.bitwise_and(zl + s, 3)
            rows[pl.ds(pl.multiple_of(at * 96, 32), 96), :] = piece.T[0:96]
    out_ref[...] = rows[...].T


def joined(place, parts):
    return pl.pallas_call(
        joined_kernel,
        in_specs=[pl.BlockSpec(memory_space=pltpu.SMEM)] + [VMEM] * 4,
        out_specs=VMEM,
        out_shape=jax.ShapeDtypeStruct((64, D), f32),
        scratch_shapes=[pltpu.VMEM((D, 64), f32)],
        compiler_params=pltpu.CompilerParams(vmem_limit_bytes=8 * 1024 * 1024),
    )(place, *parts)


def step(embeddings, fine, parents, coarse):
    core, zl, zh = (lax.axis_index(a) for a in ("core", "zl", "zh"))
    place = jnp.stack([core, zh, zl])

    own_narrow = fine.astype(bf16)
    own_norm = 0.5 * jnp.sum(fine * fine, axis=1)
    norm_part = lax.dynamic_slice_in_dim(own_norm, 256 * core, 256)
    parts = []
    for _ in range(3):
        parts.append(lax.reduce_precision(norm_part, 8, 7))
        norm_part = norm_part - parts[-1]
    last = jnp.broadcast_to(jnp.concatenate(parts).astype(bf16)[None], (8, D))
    share = jnp.concatenate([lax.dynamic_slice_in_dim(own_narrow, 256 * core, 256, 0), last])
    direct = from_ahead(share, "zh", 1)
    relayed = from_ahead(direct, "core", 1)
    cs = (direct, relayed, own_narrow)

    halves = (embeddings[:64], embeddings[64:])
    near = [jnp.concatenate(ring_of_four(h, axis)) for h, axis in zip(halves, ("x", "y"))]
    ahead = [from_ahead(b, axis, 1) for b, axis in zip(near, ("y", "x"))]
    behind = [from_ahead(b, axis, 3) for b, axis in zip(near, ("y", "x"))]
    far = [from_ahead(a, axis, 1) for a, axis in zip(ahead, ("y", "x"))]
    first = [near[0], ahead[0], behind[0], near[1], ahead[1], behind[1]]
    p0, stat, x0 = weigh(place, 0, (), first, cs, own_norm[None])
    p1, stat, x1 = weigh(place, 6, (stat,), far, cs, own_norm[None])
    weight = merged_over(merged_over(stat, "x", 0), "y", 1, own=stat)
    keep, send = weighted_sums(place, (p0, p1), weight, (x0, x1))
    tiles = (keep + from_ahead(send, "core", 1).astype(f32)) * SENT_SCALE
    arrived = lax.all_to_all(
        tiles.astype(f16).reshape(8, 104, 512), ("zh", "zl"), 0, 0, tiled=True
    )
    owned = jnp.sum(arrived.astype(f32), axis=0) / SENT_SCALE
    mass = 1.0 + owned[96:97]
    first_row = core * 384 + zl * 96
    pooled = lax.dynamic_slice_in_dim(fine, first_row, 96, 1).T + owned[:96]

    new_half = gathered_over((pooled / mass).astype(f16), "zl").reshape(384, 512)
    new_fine = gathered_over(new_half, "core").reshape(768, 512)
    new_fine = new_fine.astype(f32).T

    with_mass = jnp.concatenate([pooled, jnp.broadcast_to(mass, (32, 512))]) * SENT_SCALE
    part = pl.pallas_call(
        coarse_kernel,
        out_shape=jax.ShapeDtypeStruct((KC, 128), f32),
        compiler_params=pltpu.CompilerParams(vmem_limit_bytes=24 * 1024 * 1024),
    )(with_mass, parents[None])
    arrived = lax.all_to_all(
        part.astype(f16).reshape(32, 64, 128), ("y", "zh", "x"), 0, 0, tiled=True
    )
    total = jnp.sum(arrived.astype(f32), axis=0) / SENT_SCALE
    old = lax.dynamic_slice_in_dim(coarse, first_row, 96, 1)
    new_cols = (PRIOR * old + total[:, :96]) / (PRIOR + total[:, 96:97])
    cols = jnp.concatenate([new_cols, jnp.zeros((64, 32), f32)], axis=1)
    pair = jnp.stack([cols, from_ahead(cols, "core", 1)])
    parts = [pair] + [from_ahead(pair, "zl", s) for s in (1, 2, 3)]
    new_coarse = joined(place, parts)
    return new_fine, new_coarse


def solution(mesh):
    places = Mesh(mesh.devices.reshape(tuple(AXES.values())), tuple(AXES))
    cent = ("y", "zh", "x")
    in_specs = (P(("zl", "core", *cent), None), P(cent, None), P(cent), P(cent, None))
    out_specs = (P(cent, None), P(cent, None))
    return jax.shard_map(step, mesh=places, in_specs=in_specs, out_specs=out_specs, check_vma=False)
```

```python
import jax
import jax.numpy as jnp
from jax import lax
from jax.experimental import pallas as pl
from jax.experimental.pallas import tpu as pltpu
from jax.sharding import Mesh
from jax.sharding import PartitionSpec as P


KC = 2048
D = 768
PRIOR = 16.0
LOG2E = 1.4426950408889634
SCALE = 0.1 * LOG2E
SENT_SCALE = 1.0 / 16.0
WEIGH_MB = 24
SUMS_MB = 28
bf16, f16, f32 = jnp.bfloat16, jnp.float16, jnp.float32


AXES = {"zl": 4, "core": 2, "y": 4, "zh": 2, "x": 4}


def from_ahead(array, axis, step):
    size = AXES[axis]
    if axis not in ("x", "y"):
        return lax.ppermute(array, axis, [((me + step) % size, me) for me in range(size)])
    pairs = []
    for core in (0, 1):
        for me in range(size):
            source = (me + (step if core == 0 else -step)) % size
            pairs.append((core * size + source, core * size + me))
    return lax.ppermute(array, ("core", axis), pairs)


def z_place(z):
    return z % 4 * 2 + z // 4


def ring_of_four(array, axis):
    return [array] + [from_ahead(array, axis, s) for s in (1, 2, 3)]


VMEM = pl.BlockSpec(memory_space=pltpu.VMEM)


def weigh_kernel(first, n, *refs):
    skip = 1 if first else 0
    x_refs, c_refs, norm_ref = refs[skip : skip + n], refs[skip + n : skip + n + 3], refs[skip + n + 3]
    p_ref, stat_ref, x_all, norms = refs[skip + n + 4 :]
    if first:
        stat_ref[...] = refs[0][...]
    norms[512:1024, :] = jnp.broadcast_to(norm_ref[...], (128, 512)).T
    for at, c_ref in ((0, c_refs[0]), (256, c_refs[1])):
        row = c_ref[256:264, :].astype(f32)[0:1]
        row = row[:, 0:256] + row[:, 256:512] + row[:, 512:768]
        norms[at : at + 256, :] = jnp.broadcast_to(row, (128, 256)).T

    spans = ((0, 256), (256, 256), (512, 512))
    for i in range(n):
        x = x_refs[i][...]
        x_all[256 * i : 256 * i + 256, :] = x
        tops = []
        for (at, size), c_ref in zip(spans, c_refs):
            t = lax.dot_general(
                c_ref[0:size, :], x, (((1,), (1,)), ((), ())), preferred_element_type=f32
            )
            norm = norms[at : at + size, :]
            t = (t - jnp.concatenate([norm, norm], axis=1)) * SCALE
            p_ref[i, at : at + size, :] = t
            tops.append(jnp.max(t, axis=0, keepdims=True))
        top = jnp.maximum(jnp.maximum(tops[0], tops[1]), tops[2])
        mass = jnp.zeros((1, 256), f32)
        for at, size in spans:
            p = jnp.exp2(p_ref[i, at : at + size, :] - top)
            p_ref[i, at : at + size, :] = p
            mass = mass + jnp.sum(p, axis=0, keepdims=True)
        stat_ref[0, first + i : first + i + 1, :] = top
        stat_ref[1, first + i : first + i + 1, :] = mass


def weigh(first, stats, xs, cs, norm):
    n = len(xs)
    rows = 256 * n
    return pl.pallas_call(
        lambda *refs: weigh_kernel(first, n, *refs),
        in_specs=[VMEM] * (len(stats) + n + 4),
        out_specs=(VMEM,) * 3,
        out_shape=(
            jax.ShapeDtypeStruct((n, 1024, 256), f32),
            jax.ShapeDtypeStruct((2, 8, 256), f32),
            jax.ShapeDtypeStruct((rows, D), bf16),
        ),
        scratch_shapes=[pltpu.VMEM((1024, 128), f32)],
        cost_estimate=pl.CostEstimate(
            flops=2 * rows * 1024 * D,
            transcendentals=rows * 1024,
            bytes_accessed=2 * rows * D + 2 * 1024 * D + 4 * rows * 1024,
        ),
        compiler_params=pltpu.CompilerParams(vmem_limit_bytes=WEIGH_MB * 1024 * 1024),
    )(*stats, *xs, *cs, norm)


PIECES = ((0, 1, 6, 2), (3, 4, 7, 5))


def merge_kernel(rolled, last, *refs):
    parts, out_ref = refs[:4], refs[4]
    for half, pieces in enumerate(PIECES):
        for at, piece in enumerate(pieces):
            tops, masses = [], []
            for s, part in enumerate(parts):
                row = piece if half == rolled else pieces[(at - s) % 4]
                top, mass = part[0, row : row + 1, :], part[1, row : row + 1, :]
                if half == rolled and s:
                    cut = 256 - 64 * s
                    top = jnp.concatenate([top[:, cut:], top[:, :cut]], axis=1)
                    mass = jnp.concatenate([mass[:, cut:], mass[:, :cut]], axis=1)
                tops.append(top)
                masses.append(mass)
            high = jnp.maximum(jnp.maximum(tops[0], tops[1]), jnp.maximum(tops[2], tops[3]))
            total = sum(m * jnp.exp2(t - high) for m, t in zip(masses, tops))
            if last:
                own = refs[5][0, piece : piece + 1, :]
                out_ref[piece : piece + 1, :] = jnp.exp2(own - high) / total
            else:
                out_ref[0, piece : piece + 1, :] = high
                out_ref[1, piece : piece + 1, :] = total


def merge_last_kernel(rolled, *refs):
    merge_kernel(rolled, True, *refs[:4], refs[5], refs[4])


def merged_over(stat, axis, rolled, own=None):
    parts = [stat] + [from_ahead(stat, axis, s) for s in (1, 2, 3)]
    if own is None:
        kernel, shape = (lambda *refs: merge_kernel(rolled, False, *refs)), (2, 8, 256)
    else:
        kernel, shape = (lambda *refs: merge_last_kernel(rolled, *refs)), (8, 256)
        parts.append(own)
    return pl.pallas_call(
        kernel,
        in_specs=[VMEM] * len(parts),
        out_specs=VMEM,
        out_shape=jax.ShapeDtypeStruct(shape, f32),
        compiler_params=pltpu.CompilerParams(vmem_limit_bytes=4 * 1024 * 1024),
    )(*parts)


def sums_kernel(p0_ref, p1_ref, w_ref, x0_ref, x1_ref, keep_ref, send_ref, parts, turned):
    core, zh = lax.axis_index("core"), lax.axis_index("zh")
    first = p0_ref.shape[0]

    def one_tile(tile, carried):
        span = pl.ds(pl.multiple_of(256 * tile, 256), 256)
        count = jnp.zeros((256, 128), f32)
        for i in range(8):
            p = p0_ref[i, span, :] if i < first else p1_ref[i - first, span, :]
            soft = p * w_ref[i : i + 1, :]
            high = soft.astype(bf16)
            parts[0:256, 256 * i : 256 * i + 256] = high
            parts[256:512, 256 * i : 256 * i + 256] = (soft - high.astype(f32)).astype(bf16)
            count = count + (soft[:, :128] + soft[:, 128:])
        both = jnp.dot(parts[:, : 256 * first], x0_ref[...], preferred_element_type=f32)
        both = both + jnp.dot(parts[:, 256 * first :], x1_ref[...], preferred_element_type=f32)
        turned[...] = (both[:256] + both[256:]).T
        counted = jnp.broadcast_to(jnp.sum(count.T, axis=0, keepdims=True), (8, 256))
        side = jnp.bitwise_and(tile, 1)
        block = jnp.where(tile < 2, 1 - zh, zh)
        col = jnp.where(tile < 2, jnp.bitwise_xor(core, side), side)
        lanes = pl.ds(pl.multiple_of(col * 256, 256), 256)
        for ref, half in ((keep_ref, core), (send_ref, 1 - core)):
            for q in range(4):
                part = turned[pl.ds(pl.multiple_of(384 * half + 96 * q, 32), 96), :]
                ref[block, q, 0:96, lanes] = part
                ref[block, q, 96:104, lanes] = counted
        return carried

    lax.fori_loop(0, 4, one_tile, 0)


def weighted_sums(ps, w, xs):
    rows = 2048
    shape = jax.ShapeDtypeStruct((2, 4, 104, 512), f32)
    return pl.pallas_call(
        sums_kernel,
        in_specs=[VMEM] * 5,
        out_specs=(VMEM, VMEM),
        out_shape=(shape, shape),
        scratch_shapes=[pltpu.VMEM((512, rows), bf16), pltpu.VMEM((D, 256), f32)],
        cost_estimate=pl.CostEstimate(
            flops=8 * rows * 512 * D,
            transcendentals=0,
            bytes_accessed=2 * rows * D + 8 * rows * 512 + 8 * 832 * 512,
        ),
        compiler_params=pltpu.CompilerParams(vmem_limit_bytes=SUMS_MB * 1024 * 1024),
    )(*ps, w, *xs)


def coarse_kernel(pooled_ref, parents_ref, out_ref):
    ids = lax.broadcasted_iota(jnp.int32, (KC, 512), 0)
    hot = (ids == parents_ref[...]).astype(f32).astype(bf16)
    pooled = pooled_ref[...]
    high = pooled.astype(bf16)
    low = (pooled - high.astype(f32)).astype(bf16)
    both = lax.dot_general(
        hot,
        jnp.concatenate([high, low]),
        (((1,), (1,)), ((), ())),
        preferred_element_type=f32,
    )
    out_ref[...] = both[:, :128] + both[:, 128:]


def gathered_over(tile, axis):
    size = AXES[axis]
    me = lax.axis_index(axis)
    parts = [tile] + [from_ahead(tile, axis, s) for s in range(1, size)]
    stacked = jnp.stack(parts + parts)
    return lax.dynamic_slice_in_dim(stacked, (size - me) % size, size, 0)


def joined_kernel(*refs):
    parts, out_ref, rows = refs[:4], refs[4], refs[5]
    core, zl = lax.axis_index("core"), lax.axis_index("zl")
    for s in range(4):
        for c in (0, 1):
            piece = parts[s][c]
            at = jnp.bitwise_xor(core, c) * 4 + jnp.bitwise_and(zl + s, 3)
            rows[pl.ds(pl.multiple_of(at * 96, 32), 96), :] = piece.T[0:96]
    out_ref[...] = rows[...].T


def joined(parts):
    return pl.pallas_call(
        joined_kernel,
        in_specs=[VMEM] * 4,
        out_specs=VMEM,
        out_shape=jax.ShapeDtypeStruct((64, D), f32),
        scratch_shapes=[pltpu.VMEM((D, 64), f32)],
        compiler_params=pltpu.CompilerParams(vmem_limit_bytes=8 * 1024 * 1024),
    )(*parts)


def step(embeddings, fine, parents, coarse):
    core, zl, zh = (lax.axis_index(a) for a in ("core", "zl", "zh"))

    own_narrow = fine.astype(bf16)
    own_norm = 0.5 * jnp.sum(fine * fine, axis=1)
    norm_part = lax.dynamic_slice_in_dim(own_norm, 256 * core, 256)
    parts = []
    for _ in range(3):
        parts.append(lax.reduce_precision(norm_part, 8, 7))
        norm_part = norm_part - parts[-1]
    place = (core + 2 * zh + 4 * zl).astype(f32)
    is_norm = lax.broadcasted_iota(jnp.int32, (8, D), 0) == 0
    last = jnp.where(is_norm, jnp.concatenate(parts)[None], place).astype(bf16)
    share = jnp.concatenate([lax.dynamic_slice_in_dim(own_narrow, 256 * core, 256, 0), last])
    direct = from_ahead(share, "zh", 1)
    relayed = from_ahead(direct, "core", 1)
    cs = (direct, relayed, own_narrow)

    halves = (embeddings[:64], embeddings[64:])
    near = [jnp.concatenate(ring_of_four(h, axis)) for h, axis in zip(halves, ("x", "y"))]
    ahead = [from_ahead(b, axis, 1) for b, axis in zip(near, ("y", "x"))]
    behind = [from_ahead(b, axis, 3) for b, axis in zip(near, ("y", "x"))]
    far = [from_ahead(a, axis, 1) for a, axis in zip(ahead, ("y", "x"))]
    first = [near[0], ahead[0], behind[0], near[1], ahead[1], behind[1]]
    p0, stat, x0 = weigh(0, (), first, cs, own_norm[None])
    p1, stat, x1 = weigh(6, (stat,), far, cs, own_norm[None])
    weight = merged_over(merged_over(stat, "x", 0), "y", 1, own=stat)
    keep, send = weighted_sums((p0, p1), weight, (x0, x1))
    tiles = (keep + from_ahead(send, "core", 1).astype(f32)) * SENT_SCALE
    tiles = tiles.astype(f16).reshape(8, 104, 512)
    z = zh * 4 + zl
    owned = lax.dynamic_index_in_dim(tiles, z, 0, keepdims=False).astype(f32)
    for s in (4, 3, 5, 2, 6, 1, 7):
        sent = lax.dynamic_index_in_dim(tiles, jnp.bitwise_and(z - s, 7), 0, keepdims=False)
        pairs = [(z_place((me + s) % 8), z_place(me)) for me in range(8)]
        owned = owned + lax.ppermute(sent, ("zl", "zh"), pairs).astype(f32)
    owned = owned / SENT_SCALE
    mass = 1.0 + owned[96:97]
    first_row = core * 384 + zl * 96
    pooled = lax.dynamic_slice_in_dim(fine, first_row, 96, 1).T + owned[:96]

    new_half = gathered_over((pooled / mass).astype(f16), "zl").reshape(384, 512)
    new_fine = gathered_over(new_half, "core").reshape(768, 512)
    new_fine = new_fine.astype(f32).T

    with_mass = jnp.concatenate([pooled, jnp.broadcast_to(mass, (32, 512))]) * SENT_SCALE
    part = pl.pallas_call(
        coarse_kernel,
        out_shape=jax.ShapeDtypeStruct((KC, 128), f32),
        compiler_params=pltpu.CompilerParams(vmem_limit_bytes=24 * 1024 * 1024),
    )(with_mass, parents[None])
    arrived = lax.all_to_all(
        part.astype(f16).reshape(32, 64, 128), ("y", "zh", "x"), 0, 0, tiled=True
    )
    total = jnp.sum(arrived.astype(f32), axis=0) / SENT_SCALE
    old = lax.dynamic_slice_in_dim(coarse, first_row, 96, 1)
    new_cols = (PRIOR * old + total[:, :96]) / (PRIOR + total[:, 96:97])
    cols = jnp.concatenate([new_cols, jnp.zeros((64, 32), f32)], axis=1)
    pair = jnp.stack([cols, from_ahead(cols, "core", 1)])
    parts = [pair] + [from_ahead(pair, "zl", s) for s in (1, 2, 3)]
    new_coarse = joined(parts)
    return new_fine, new_coarse


def solution(mesh):
    places = Mesh(mesh.devices.reshape(tuple(AXES.values())), tuple(AXES))
    cent = ("y", "zh", "x")
    in_specs = (P(("zl", "core", *cent), None), P(cent, None), P(cent), P(cent, None))
    out_specs = (P(cent, None), P(cent, None))
    return jax.shard_map(step, mesh=places, in_specs=in_specs, out_specs=out_specs, check_vma=False)
```

```python
import jax
import jax.numpy as jnp
from jax import lax
from jax.experimental import pallas as pl
from jax.experimental.pallas import tpu as pltpu
from jax.sharding import Mesh
from jax.sharding import PartitionSpec as P


KC = 2048
D = 768
PRIOR = 16.0
LOG2E = 1.4426950408889634
SCALE = 0.1 * LOG2E
SENT_SCALE = 1.0 / 16.0
WEIGH_MB = 24
SUMS_MB = 28
bf16, f16, f32 = jnp.bfloat16, jnp.float16, jnp.float32


AXES = {"zl": 4, "core": 2, "y": 4, "zh": 2, "x": 4}


def from_ahead(array, axis, step):
    size = AXES[axis]
    if axis not in ("x", "y"):
        return lax.ppermute(array, axis, [((me + step) % size, me) for me in range(size)])
    pairs = []
    for core in (0, 1):
        for me in range(size):
            source = (me + (step if core == 0 else -step)) % size
            pairs.append((core * size + source, core * size + me))
    return lax.ppermute(array, ("core", axis), pairs)


def ring_of_four(array, axis):
    return [array] + [from_ahead(array, axis, s) for s in (1, 2, 3)]


VMEM = pl.BlockSpec(memory_space=pltpu.VMEM)


def weigh_kernel(first, n, *refs):
    skip = 1 if first else 0
    x_refs, c_refs, norm_ref = refs[skip : skip + n], refs[skip + n : skip + n + 3], refs[skip + n + 3]
    p_ref, stat_ref, x_all, norms = refs[skip + n + 4 :]
    if first:
        stat_ref[...] = refs[0][...]
    norms[512:1024, :] = jnp.broadcast_to(norm_ref[...], (128, 512)).T
    for at, c_ref in ((0, c_refs[0]), (256, c_refs[1])):
        row = c_ref[256:264, :].astype(f32)[0:1]
        row = row[:, 0:256] + row[:, 256:512] + row[:, 512:768]
        norms[at : at + 256, :] = jnp.broadcast_to(row, (128, 256)).T

    for i in range(n):
        x_all[256 * i : 256 * i + 256, :] = x_refs[i][...]

    spans = ((0, 256), (256, 256), (512, 512))

    def piece(i, carried):
        x = x_all[pl.ds(pl.multiple_of(256 * i, 256), 256), :]
        tops = []
        for (at, size), c_ref in zip(spans, c_refs):
            t = lax.dot_general(
                c_ref[0:size, :], x, (((1,), (1,)), ((), ())), preferred_element_type=f32
            )
            norm = norms[at : at + size, :]
            t = (t - jnp.concatenate([norm, norm], axis=1)) * SCALE
            p_ref[i, at : at + size, :] = t
            tops.append(jnp.max(t, axis=0, keepdims=True))
        top = jnp.maximum(jnp.maximum(tops[0], tops[1]), tops[2])
        mass = jnp.zeros((1, 256), f32)
        for at, size in spans:
            p = jnp.exp2(p_ref[i, at : at + size, :] - top)
            p_ref[i, at : at + size, :] = p
            mass = mass + jnp.sum(p, axis=0, keepdims=True)
        stat_ref[0, pl.ds(first + i, 1), :] = top
        stat_ref[1, pl.ds(first + i, 1), :] = mass
        return carried

    lax.fori_loop(0, n // 2, lambda i, c: piece(2 * i + 1, piece(2 * i, c)), 0)


def weigh(first, stats, xs, cs, norm):
    n = len(xs)
    rows = 256 * n
    return pl.pallas_call(
        lambda *refs: weigh_kernel(first, n, *refs),
        in_specs=[VMEM] * (len(stats) + n + 4),
        out_specs=(VMEM,) * 3,
        out_shape=(
            jax.ShapeDtypeStruct((n, 1024, 256), f32),
            jax.ShapeDtypeStruct((2, 8, 256), f32),
            jax.ShapeDtypeStruct((rows, D), bf16),
        ),
        scratch_shapes=[pltpu.VMEM((1024, 128), f32)],
        cost_estimate=pl.CostEstimate(
            flops=2 * rows * 1024 * D,
            transcendentals=rows * 1024,
            bytes_accessed=2 * rows * D + 2 * 1024 * D + 4 * rows * 1024,
        ),
        compiler_params=pltpu.CompilerParams(vmem_limit_bytes=WEIGH_MB * 1024 * 1024),
    )(*stats, *xs, *cs, norm)


PIECES = ((0, 1, 6, 2), (3, 4, 7, 5))


def merge_kernel(rolled, last, *refs):
    parts, out_ref = refs[:4], refs[4]
    for half, pieces in enumerate(PIECES):
        for at, piece in enumerate(pieces):
            tops, masses = [], []
            for s, part in enumerate(parts):
                row = piece if half == rolled else pieces[(at - s) % 4]
                top, mass = part[0, row : row + 1, :], part[1, row : row + 1, :]
                if half == rolled and s:
                    cut = 256 - 64 * s
                    top = jnp.concatenate([top[:, cut:], top[:, :cut]], axis=1)
                    mass = jnp.concatenate([mass[:, cut:], mass[:, :cut]], axis=1)
                tops.append(top)
                masses.append(mass)
            high = jnp.maximum(jnp.maximum(tops[0], tops[1]), jnp.maximum(tops[2], tops[3]))
            total = sum(m * jnp.exp2(t - high) for m, t in zip(masses, tops))
            if last:
                own = refs[5][0, piece : piece + 1, :]
                out_ref[piece : piece + 1, :] = jnp.exp2(own - high) / total
            else:
                out_ref[0, piece : piece + 1, :] = high
                out_ref[1, piece : piece + 1, :] = total


def merge_last_kernel(rolled, *refs):
    merge_kernel(rolled, True, *refs[:4], refs[5], refs[4])


def merged_over(stat, axis, rolled, own=None):
    parts = [stat] + [from_ahead(stat, axis, s) for s in (1, 2, 3)]
    if own is None:
        kernel, shape = (lambda *refs: merge_kernel(rolled, False, *refs)), (2, 8, 256)
    else:
        kernel, shape = (lambda *refs: merge_last_kernel(rolled, *refs)), (8, 256)
        parts.append(own)
    return pl.pallas_call(
        kernel,
        in_specs=[VMEM] * len(parts),
        out_specs=VMEM,
        out_shape=jax.ShapeDtypeStruct(shape, f32),
        compiler_params=pltpu.CompilerParams(vmem_limit_bytes=4 * 1024 * 1024),
    )(*parts)


def sums_kernel(away, p0_ref, p1_ref, w_ref, x0_ref, x1_ref, keep_ref, send_ref, parts, turned):
    core, zl = lax.axis_index("core"), lax.axis_index("zl")
    first = p0_ref.shape[0]

    def one_tile(tile, carried):
        span = pl.ds(pl.multiple_of(256 * tile + (0 if away else 512), 256), 256)
        count = jnp.zeros((256, 128), f32)
        for i in range(8):
            p = p0_ref[i, span, :] if i < first else p1_ref[i - first, span, :]
            soft = p * w_ref[i : i + 1, :]
            high = soft.astype(bf16)
            parts[0:256, 256 * i : 256 * i + 256] = high
            parts[256:512, 256 * i : 256 * i + 256] = (soft - high.astype(f32)).astype(bf16)
            count = count + (soft[:, :128] + soft[:, 128:])
        both = jnp.dot(parts[:, : 256 * first], x0_ref[...], preferred_element_type=f32)
        both = both + jnp.dot(parts[:, 256 * first :], x1_ref[...], preferred_element_type=f32)
        turned[...] = (both[:256] + both[256:]).T
        counted = jnp.broadcast_to(jnp.sum(count.T, axis=0, keepdims=True), (8, 256))
        col = jnp.bitwise_xor(core, tile) if away else tile
        lanes = pl.ds(pl.multiple_of(col * 256, 256), 256)
        for ref, half in ((keep_ref, core), (send_ref, 1 - core)):
            for behind in range(4):
                q = jnp.bitwise_and(zl - behind, 3)
                part = turned[pl.ds(pl.multiple_of(384 * half + 96 * q, 32), 96), :]
                ref[behind, 0:96, lanes] = part
                ref[behind, 96:104, lanes] = counted
        return carried

    lax.fori_loop(0, 2, one_tile, 0)


def weighted_sums(away, ps, w, xs):
    rows = 2048
    shape = jax.ShapeDtypeStruct((4, 104, 512), f32)
    return pl.pallas_call(
        lambda *refs: sums_kernel(away, *refs),
        in_specs=[VMEM] * 5,
        out_specs=(VMEM, VMEM),
        out_shape=(shape, shape),
        scratch_shapes=[pltpu.VMEM((512, rows), bf16), pltpu.VMEM((D, 256), f32)],
        cost_estimate=pl.CostEstimate(
            flops=4 * rows * 512 * D,
            transcendentals=0,
            bytes_accessed=2 * rows * D + 4 * rows * 512 + 4 * 832 * 512,
        ),
        compiler_params=pltpu.CompilerParams(vmem_limit_bytes=SUMS_MB * 1024 * 1024),
    )(*ps, w, *xs)


def coarse_kernel(pooled_ref, parents_ref, out_ref):
    ids = lax.broadcasted_iota(jnp.int32, (KC, 512), 0)
    hot = (ids == parents_ref[...]).astype(f32).astype(bf16)
    pooled = pooled_ref[...]
    high = pooled.astype(bf16)
    low = (pooled - high.astype(f32)).astype(bf16)
    both = lax.dot_general(
        hot,
        jnp.concatenate([high, low]),
        (((1,), (1,)), ((), ())),
        preferred_element_type=f32,
    )
    out_ref[...] = both[:, :128] + both[:, 128:]


def gathered_over(tile, axis):
    size = AXES[axis]
    me = lax.axis_index(axis)
    parts = [tile] + [from_ahead(tile, axis, s) for s in range(1, size)]
    stacked = jnp.stack(parts + parts)
    return lax.dynamic_slice_in_dim(stacked, (size - me) % size, size, 0)


def joined_kernel(*refs):
    parts, out_ref, rows = refs[:4], refs[4], refs[5]
    core, zl = lax.axis_index("core"), lax.axis_index("zl")
    for s in range(4):
        for c in (0, 1):
            piece = parts[s][c]
            at = jnp.bitwise_xor(core, c) * 4 + jnp.bitwise_and(zl + s, 3)
            rows[pl.ds(pl.multiple_of(at * 96, 32), 96), :] = piece.T[0:96]
    out_ref[...] = rows[...].T


def joined(parts):
    return pl.pallas_call(
        joined_kernel,
        in_specs=[VMEM] * 4,
        out_specs=VMEM,
        out_shape=jax.ShapeDtypeStruct((64, D), f32),
        scratch_shapes=[pltpu.VMEM((D, 64), f32)],
        compiler_params=pltpu.CompilerParams(vmem_limit_bytes=8 * 1024 * 1024),
    )(*parts)


def step(embeddings, fine, parents, coarse):
    core, zl, zh = (lax.axis_index(a) for a in ("core", "zl", "zh"))

    own_narrow = fine.astype(bf16)
    own_norm = 0.5 * jnp.sum(fine * fine, axis=1)
    norm_part = lax.dynamic_slice_in_dim(own_norm, 256 * core, 256)
    parts = []
    for _ in range(3):
        parts.append(lax.reduce_precision(norm_part, 8, 7))
        norm_part = norm_part - parts[-1]
    place = (core + 2 * zh + 4 * zl).astype(f32)
    is_norm = lax.broadcasted_iota(jnp.int32, (8, D), 0) == 0
    last = jnp.where(is_norm, jnp.concatenate(parts)[None], place).astype(bf16)
    share = jnp.concatenate([lax.dynamic_slice_in_dim(own_narrow, 256 * core, 256, 0), last])
    direct = from_ahead(share, "zh", 1)
    relayed = from_ahead(direct, "core", 1)
    cs = (direct, relayed, own_narrow)

    halves = (embeddings[:64], embeddings[64:])
    near = [jnp.concatenate(ring_of_four(h, axis)) for h, axis in zip(halves, ("x", "y"))]
    ahead = [from_ahead(b, axis, 1) for b, axis in zip(near, ("y", "x"))]
    behind = [from_ahead(b, axis, 3) for b, axis in zip(near, ("y", "x"))]
    far = []
    for a, axis in zip(ahead, ("y", "x")):
        far.append(from_ahead(a, axis, 1))
    first = [near[0], ahead[0], behind[0], near[1], ahead[1], behind[1]]
    p0, stat, x0 = weigh(0, (), first, cs, own_norm[None])
    p1, stat, x1 = weigh(6, (stat,), far, cs, own_norm[None])
    weight = merged_over(merged_over(stat, "x", 0), "y", 1, own=stat)
    keep, send = weighted_sums(True, (p0, p1), weight, (x0, x1))
    tiles = ((keep + from_ahead(send, "core", 1)) * SENT_SCALE).astype(f16)
    arrived = []
    for s in (0, 1, 3, 2):
        pairs = [((zl_ + s) % 4 * 2 + 1 - zh_, zl_ * 2 + zh_) for zl_ in range(4) for zh_ in (0, 1)]
        arrived.append(lax.ppermute(tiles[s], ("zl", "zh"), pairs))
    keep, send = weighted_sums(False, (p0, p1), weight, (x0, x1))
    other = from_ahead(send, "core", 1)
    tiles = ((keep + other) * SENT_SCALE).astype(f16)
    for s in (1, 3, 2):
        arrived.append(from_ahead(tiles[s], "zl", s))
    owned = sum((a.astype(f32) for a in arrived), tiles[0].astype(f32)) / SENT_SCALE
    mass = 1.0 + owned[96:97]
    first_row = core * 384 + zl * 96
    pooled = lax.dynamic_slice_in_dim(fine, first_row, 96, 1).T + owned[:96]

    new_half = gathered_over((pooled / mass).astype(f16), "zl").reshape(384, 512)
    new_fine = gathered_over(new_half, "core").reshape(768, 512)
    new_fine = new_fine.astype(f32).T

    with_mass = jnp.concatenate([pooled, jnp.broadcast_to(mass, (32, 512))]) * SENT_SCALE
    part = pl.pallas_call(
        coarse_kernel,
        out_shape=jax.ShapeDtypeStruct((KC, 128), f32),
        compiler_params=pltpu.CompilerParams(vmem_limit_bytes=24 * 1024 * 1024),
    )(with_mass, parents[None])
    arrived = lax.all_to_all(
        part.astype(f16).reshape(32, 64, 128), ("y", "zh", "x"), 0, 0, tiled=True
    )
    total = jnp.sum(arrived.astype(f32), axis=0) / SENT_SCALE
    old = lax.dynamic_slice_in_dim(coarse, first_row, 96, 1)
    new_cols = (PRIOR * old + total[:, :96]) / (PRIOR + total[:, 96:97])
    cols = jnp.concatenate([new_cols, jnp.zeros((64, 32), f32)], axis=1)
    pair = jnp.stack([cols, from_ahead(cols, "core", 1)])
    parts = [pair] + [from_ahead(pair, "zl", s) for s in (1, 2, 3)]
    new_coarse = joined(parts)
    return new_fine, new_coarse


def solution(mesh):
    places = Mesh(mesh.devices.reshape(tuple(AXES.values())), tuple(AXES))
    cent = ("y", "zh", "x")
    in_specs = (P(("zl", "core", *cent), None), P(cent, None), P(cent), P(cent, None))
    out_specs = (P(cent, None), P(cent, None))
    return jax.shard_map(step, mesh=places, in_specs=in_specs, out_specs=out_specs, check_vma=False)
```
